32 devices in a mesh: bank: 4 (over z), zero: 8 (over y, x, core).
Axes of the slice: x: 2, y: 2, z: 4, core: 2. Of those that a mesh axis runs over, the one named last changes fastest.
Arguments:
- w_gate: float32 [128, 2048, 768], P('bank', 'zero'), may hold values from -0.1875 to 0.1875
- w_up: float32 [128, 2048, 768], P('bank', 'zero'), may hold values from -0.1875 to 0.1875
- router_weight: float32 [2048, 128], P('zero', 'bank'), may hold values from -0.125 to 0.125
- router_gain: float32 [2048], P('zero'), may hold values from 0.25 to 1.75
Outputs:
- serve_gate: bfloat16 [128, 2048, 768], P('bank', None, 'zero')
- serve_up: bfloat16 [128, 2048, 768], P('bank', None, 'zero')
- scale_gate: float32 [128, 768], P('bank', 'zero')
- scale_up: float32 [128, 768], P('bank', 'zero')
- serve_router: bfloat16 [2048, 128], replicated
The draws below stay inside these ranges and needn't reach their ends.
All inputs are finite; a program needn't handle non-finite values.
Results may differ from the reference program's by a relative error of at most 0.001.
Values may be sent and summed in bfloat16 or wider, within the bound.
A program may use at most 192 MiB of HBM per device.

```python
import jax
import jax.numpy as jnp
from jax import lax

EXPERTS = 128
D_MODEL = 2048
D_EXPERT = 768


def strengthened(drawn, own_key, source, target, shards_of, factor):
    owner, partner = [(jnp.arange(drawn.shape[position]) // (drawn.shape[position] // shards_of)).reshape([-1 if axis == position else 1 for axis in range(drawn.ndim)]) for position in (source, target)]
    chosen = jax.random.permutation(own_key, shards_of)[partner]
    strong = (owner == chosen) | (owner == (partner + shards_of // 2) % shards_of)
    return jnp.where(strong, factor * drawn, drawn)


def block_levels(key, shape, shards, least, top_value):
    gain, own = 1.0, jax.random.fold_in(key, 6)
    for dim, blocks in shards:
        steps = jnp.exp(jax.random.uniform(jax.random.fold_in(own, dim), (blocks,), jnp.float32, least / len(shards), top_value / len(shards)))
        gain = gain * jnp.repeat(steps, shape[dim] // blocks).reshape([-1 if axis == dim else 1 for axis in range(len(shape))])
    return gain


def noise(stream_key, shape, spread, limit, cuts=(), dtype=jnp.bfloat16):
    result = jax.random.normal(stream_key, shape, jnp.float32) * spread
    if len(cuts) > 0:
        result = block_levels(stream_key, shape, cuts, -0.22, 0.18) * result
    return jnp.clip(result, min=-limit, max=limit).astype(dtype)


def bell_draw_with(key, extent, scale, limit, shards, heavy, held_as=jnp.bfloat16):
    drawn = scale * jax.random.normal(key, extent, jnp.float32)
    if shards:
        drawn = drawn * block_levels(key, extent, shards, -0.22, 0.18)
    return jnp.clip(strengthened(drawn, jax.random.fold_in(key, 3), *heavy), -limit, limit).astype(held_as)


def setup_inputs(seed: int = 0) -> dict:
    streams_of = jax.random.split(jax.random.key(seed), 5)
    return {
        "w_gate": bell_draw_with(streams_of[0], (EXPERTS, D_MODEL, D_EXPERT), D_MODEL ** -0.5, 0.1875, ((0, 4), (1, 8)), (1, 2, 8, 2.0), jnp.float32),
        "w_up": bell_draw_with(streams_of[1], (EXPERTS, D_MODEL, D_EXPERT), D_MODEL ** -0.5, 0.1875, ((0, 4), (1, 8)), (1, 2, 8, 2.0), jnp.float32),
        "router_weight": noise(streams_of[2], (D_MODEL, EXPERTS), D_MODEL ** -0.5, 0.125, ((0, 8), (1, 4)), jnp.float32),
        "router_gain": jnp.clip(1.0 + 0.15 * jax.random.normal(streams_of[3], (D_MODEL,), jnp.float32), 0.25, 1.75),
    }


def reference(w_gate, w_up, router_weight, router_gain):
    scale_gate = jnp.sqrt(lax.optimization_barrier(jnp.sum(w_gate * w_gate, axis=1)))
    serve_gate = (w_gate / jnp.expand_dims(scale_gate, 1)).astype(jnp.bfloat16)
    scale_up = jnp.sqrt(lax.optimization_barrier(jnp.sum(w_up * w_up, axis=1)))
    serve_up = (w_up / jnp.expand_dims(scale_up, 1)).astype(jnp.bfloat16)
    serve_router = (router_weight * router_gain[:, None]).astype(jnp.bfloat16)
    return (serve_gate, serve_up, scale_gate, scale_up, serve_router)
```

```python
import functools

import jax
import jax.numpy as jnp
from jax import lax
from jax.experimental import pallas as pl
from jax.experimental.pallas import tpu as pltpu
from jax.sharding import PartitionSpec as P


def prepare_kernel(parts, w_ref, scale_ref, out_ref):
    normal = w_ref[0] / scale_ref[0]
    turned = normal.T
    width = turned.shape[0] // parts
    for part in range(parts):
        out_ref[part, 0] = turned[part * width : (part + 1) * width].astype(jnp.bfloat16)


def prepare(w, scale, parts, first, count):
    _, rows, columns = w.shape
    width = columns // parts
    return pl.pallas_call(
        functools.partial(prepare_kernel, parts),
        grid=(count,),
        in_specs=[
            pl.BlockSpec((1, rows, columns), lambda e: (e + first, 0, 0)),
            pl.BlockSpec((1, 1, columns), lambda e: (e + first, 0, 0)),
        ],
        out_specs=pl.BlockSpec((parts, 1, width, rows), lambda e: (0, e, 0, 0)),
        out_shape=jax.ShapeDtypeStruct((parts, count, width, rows), jnp.bfloat16),
        cost_estimate=pl.CostEstimate(
            flops=count * rows * columns * 40,
            bytes_accessed=count * rows * columns * 6,
            transcendentals=0,
        ),
        compiler_params=pltpu.CompilerParams(vmem_limit_bytes=32 * 2**20),
        name="prepare",
    )(w, scale[:, None, :])


def merge_kernel(parts, block_ref, *refs):
    out_ref = refs[-1]
    rows = block_ref.shape[3]
    for part in range(parts):
        out_ref[0, :, part * rows : (part + 1) * rows] = block_ref[part, 0]


def merge(blocks, before, experts, first):
    parts, count, width, rows = blocks.shape
    chained = before is not None
    return pl.pallas_call(
        functools.partial(merge_kernel, parts),
        grid=(count,),
        in_specs=[pl.BlockSpec((parts, 1, width, rows), lambda e: (0, e, 0, 0))]
        + [pl.BlockSpec(memory_space=pl.ANY)] * chained,
        out_specs=pl.BlockSpec((1, width, parts * rows), lambda e: (e + first, 0, 0)),
        out_shape=jax.ShapeDtypeStruct((experts, width, parts * rows), jnp.bfloat16),
        input_output_aliases={1: 0} if chained else {},
        cost_estimate=pl.CostEstimate(
            flops=count * rows * width * parts * 10,
            bytes_accessed=count * rows * width * parts * 4,
            transcendentals=0,
        ),
        compiler_params=pltpu.CompilerParams(vmem_limit_bytes=32 * 2**20),
        name="merge",
    )(blocks, *([before] if chained else []))


def cuts(experts, small_first):
    small = max(experts // 4, 1)
    sizes = [small, experts - small] if small_first else [experts - small, small]
    return [size for size in sizes if size]


def shards_blocked(parts, w_gate, w_up, router_weight, router_gain):
    experts, rows, columns = w_gate.shape
    width = columns // parts
    sums = jnp.stack(
        [jnp.sum(w_gate * w_gate, axis=1), jnp.sum(w_up * w_up, axis=1)]
    ).reshape(2 * experts, parts, width)
    pieces = lax.all_to_all(
        sums.transpose(1, 0, 2), "zero", split_axis=0, concat_axis=0, tiled=True
    )
    own = jnp.sqrt(jnp.sum(pieces, axis=0))
    scale_gate, scale_up = own[:experts], own[experts:]

    part_router = (router_weight * router_gain[:, None]).astype(jnp.bfloat16)
    packed = jnp.concatenate(
        [own.reshape(-1), part_router.astype(jnp.float32).reshape(-1)]
    ).reshape(1, -1, 128)
    gathered = lax.all_gather(packed, "zero", axis=0, tiled=True).reshape(parts, -1)
    scales = gathered[:, : own.size].reshape(parts, 2 * experts, width)
    scales = scales.transpose(1, 0, 2).reshape(2 * experts, columns)
    row_router = gathered[:, own.size :].reshape(parts * rows, -1).astype(jnp.bfloat16)

    results, last = [], None
    for w, scale, small_first in ((w_gate, scales[:experts], True), (w_up, scales[experts:], False)):
        first, result = 0, None
        for count in cuts(experts, small_first):
            last = prepare(w, scale, parts, first, count)
            blocks = lax.all_to_all(last, "zero", split_axis=0, concat_axis=0, tiled=True)
            result = merge(blocks, result, experts, first)
            first += count
        results.append(result.transpose(0, 2, 1))
    row_router, _ = lax.optimization_barrier((row_router, last))
    serve_router = lax.all_gather(row_router, "bank", axis=1, tiled=True)
    return (*results, scale_gate, scale_up, serve_router)


def shards_plain(w_gate, w_up, router_weight, router_gain):
    total_gate, total_up = lax.psum(
        (jnp.sum(w_gate * w_gate, axis=1), jnp.sum(w_up * w_up, axis=1)), "zero"
    )
    results, own = [], []
    for w, total in ((w_gate, total_gate), (w_up, total_up)):
        scale = jnp.sqrt(total)
        narrow = (w / jnp.expand_dims(scale, 1)).astype(jnp.bfloat16)
        serve = lax.all_to_all(narrow, "zero", split_axis=2, concat_axis=1, tiled=True)
        width = serve.shape[2]
        results.append(serve)
        own.append(
            lax.dynamic_slice_in_dim(scale, lax.axis_index("zero") * width, width, axis=1)
        )
    part_router = (router_weight * router_gain[:, None]).astype(jnp.bfloat16)
    row_router = lax.all_gather(part_router, "zero", axis=0, tiled=True)
    serve_router = lax.all_gather(row_router, "bank", axis=1, tiled=True)
    return (*results, *own, serve_router)


def solution(mesh):
    parts, banks = mesh.shape["zero"], mesh.shape["bank"]
    placed = (P("bank", "zero", None), P("bank", "zero", None), P("zero", "bank"), P("zero"))

    def shards(w_gate, w_up, router_weight, router_gain):
        experts, rows, columns = w_gate.shape
        width = columns // parts
        packed = 2 * experts * width + router_weight.size
        if rows % 128 == 0 and width % 16 == 0 and packed % 128 == 0:
            return shards_blocked(parts, w_gate, w_up, router_weight, router_gain)
        return shards_plain(w_gate, w_up, router_weight, router_gain)

    return jax.shard_map(
        shards,
        mesh=mesh,
        in_specs=placed,
        out_specs=(
            P("bank", None, "zero"),
            P("bank", None, "zero"),
            P("bank", "zero"),
            P("bank", "zero"),
            P(),
        ),
        check_vma=False,
    )
```

```python
import functools

import jax
import jax.numpy as jnp
from jax import lax
from jax.experimental import pallas as pl
from jax.experimental.pallas import tpu as pltpu
from jax.sharding import PartitionSpec as P


def prepare_kernel(parts, w_ref, scale_ref, *refs):
    out_ref = refs[-1]
    normal = w_ref[0] / scale_ref[0]
    turned = normal.T
    width = turned.shape[0] // parts
    for part in range(parts):
        out_ref[part, 0] = turned[part * width : (part + 1) * width].astype(jnp.bfloat16)


def prepare(w, scale, parts, first, count, after):
    _, rows, columns = w.shape
    width = columns // parts
    return pl.pallas_call(
        functools.partial(prepare_kernel, parts),
        grid=(count,),
        in_specs=[
            pl.BlockSpec((1, rows, columns), lambda e: (e + first, 0, 0)),
            pl.BlockSpec((1, 1, columns), lambda e: (e + first, 0, 0)),
        ]
        + [pl.BlockSpec(memory_space=pl.ANY)] * len(after),
        out_specs=pl.BlockSpec((parts, 1, width, rows), lambda e: (0, e, 0, 0)),
        out_shape=jax.ShapeDtypeStruct((parts, count, width, rows), jnp.bfloat16),
        cost_estimate=pl.CostEstimate(
            flops=count * rows * columns * 40,
            bytes_accessed=count * rows * columns * 6,
            transcendentals=0,
        ),
        compiler_params=pltpu.CompilerParams(vmem_limit_bytes=56 * 2**20),
        name="prepare",
    )(w, scale[:, None, :], *after)


def merge_kernel(parts, block_ref, *refs):
    out_ref, token_ref = refs[-2:]
    token_ref[...] = jnp.zeros_like(token_ref)
    rows = block_ref.shape[3]
    for part in range(parts):
        out_ref[0, :, part * rows : (part + 1) * rows] = block_ref[part, 0]


def merge(blocks, before, experts, first):
    parts, count, width, rows = blocks.shape
    chained = before is not None
    return pl.pallas_call(
        functools.partial(merge_kernel, parts),
        grid=(count,),
        in_specs=[pl.BlockSpec((parts, 1, width, rows), lambda e: (0, e, 0, 0))]
        + [pl.BlockSpec(memory_space=pl.ANY)] * chained,
        out_specs=[
            pl.BlockSpec((1, width, parts * rows), lambda e: (e + first, 0, 0)),
            pl.BlockSpec((8, 128), lambda e: (0, 0)),
        ],
        out_shape=[
            jax.ShapeDtypeStruct((experts, width, parts * rows), jnp.bfloat16),
            jax.ShapeDtypeStruct((8, 128), jnp.float32),
        ],
        input_output_aliases={1: 0} if chained else {},
        cost_estimate=pl.CostEstimate(
            flops=count * rows * width * parts * 10,
            bytes_accessed=count * rows * width * parts * 4,
            transcendentals=0,
        ),
        compiler_params=pltpu.CompilerParams(vmem_limit_bytes=56 * 2**20),
        name="merge",
    )(blocks, *([before] if chained else []))


def cuts(experts, small_first):
    small = max(experts * 3 // 16, 1)
    sizes = [small, experts - small] if small_first else [experts - small, small]
    return [size for size in sizes if size]


def shards_blocked(parts, w_gate, w_up, router_weight, router_gain):
    experts, rows, columns = w_gate.shape
    width = columns // parts
    sums = jnp.stack(
        [jnp.sum(w_gate * w_gate, axis=1), jnp.sum(w_up * w_up, axis=1)]
    ).reshape(2 * experts, parts, width)
    pieces = lax.all_to_all(
        sums.transpose(1, 0, 2), "zero", split_axis=0, concat_axis=0, tiled=True
    )
    own = jnp.sqrt(jnp.sum(pieces, axis=0))
    scale_gate, scale_up = own[:experts], own[experts:]

    part_router = (router_weight * router_gain[:, None]).astype(jnp.bfloat16)
    packed = jnp.concatenate(
        [own.reshape(-1), part_router.astype(jnp.float32).reshape(-1)]
    ).reshape(1, -1, 128)
    gathered = lax.all_gather(packed, "zero", axis=0, tiled=True).reshape(parts, -1)
    scales = gathered[:, : own.size].reshape(parts, 2 * experts, width)
    scales = scales.transpose(1, 0, 2).reshape(2 * experts, columns)
    row_router = gathered[:, own.size :].reshape(parts * rows, -1).astype(jnp.bfloat16)

    chunks = [(0, count) for count in cuts(experts, True)]
    chunks += [(1, count) for count in cuts(experts, False)]
    weights, scaled = (w_gate, w_up), (scales[:experts], scales[experts:])
    first, results, tokens, serve_router = [0, 0], [None, None], [], None
    for step, (which, count) in enumerate(chunks):
        after = tokens[step - 2 : step - 1] if step >= 2 else []
        if step == len(chunks) - 1:
            row_router, *after = lax.optimization_barrier((row_router, *after))
            serve_router = lax.all_gather(row_router, "bank", axis=1, tiled=True)
            after = [*after, serve_router]
        pieces = prepare(weights[which], scaled[which], parts, first[which], count, after)
        blocks = lax.all_to_all(pieces, "zero", split_axis=0, concat_axis=0, tiled=True)
        results[which], token = merge(blocks, results[which], experts, first[which])
        tokens.append(token)
        first[which] += count
    return (
        *(result.transpose(0, 2, 1) for result in results),
        scale_gate,
        scale_up,
        serve_router,
    )


def shards_plain(w_gate, w_up, router_weight, router_gain):
    total_gate, total_up = lax.psum(
        (jnp.sum(w_gate * w_gate, axis=1), jnp.sum(w_up * w_up, axis=1)), "zero"
    )
    results, own = [], []
    for w, total in ((w_gate, total_gate), (w_up, total_up)):
        scale = jnp.sqrt(total)
        narrow = (w / jnp.expand_dims(scale, 1)).astype(jnp.bfloat16)
        serve = lax.all_to_all(narrow, "zero", split_axis=2, concat_axis=1, tiled=True)
        width = serve.shape[2]
        results.append(serve)
        own.append(
            lax.dynamic_slice_in_dim(scale, lax.axis_index("zero") * width, width, axis=1)
        )
    part_router = (router_weight * router_gain[:, None]).astype(jnp.bfloat16)
    row_router = lax.all_gather(part_router, "zero", axis=0, tiled=True)
    serve_router = lax.all_gather(row_router, "bank", axis=1, tiled=True)
    return (*results, *own, serve_router)


def solution(mesh):
    parts, banks = mesh.shape["zero"], mesh.shape["bank"]
    placed = (P("bank", "zero", None), P("bank", "zero", None), P("zero", "bank"), P("zero"))

    def shards(w_gate, w_up, router_weight, router_gain):
        experts, rows, columns = w_gate.shape
        width = columns // parts
        packed = 2 * experts * width + router_weight.size
        if rows % 128 == 0 and width % 16 == 0 and packed % 128 == 0:
            return shards_blocked(parts, w_gate, w_up, router_weight, router_gain)
        return shards_plain(w_gate, w_up, router_weight, router_gain)

    return jax.shard_map(
        shards,
        mesh=mesh,
        in_specs=placed,
        out_specs=(
            P("bank", None, "zero"),
            P("bank", None, "zero"),
            P("bank", "zero"),
            P("bank", "zero"),
            P(),
        ),
        check_vma=False,
    )
```
